32 devices in a mesh: dp: 8 (over z, x), tensor: 4 (over y, core).
Axes of the slice: x: 2, y: 2, z: 4, core: 2. Of those that a mesh axis runs over, the one named last changes fastest.
Arguments:
- logits: bfloat16 [16, 128, 19456], P('dp', None, 'tensor'), may hold values from -110 to 290
- token_ids: int32 [16, 128], P('dp'), may hold values from 0 to 19455
- response_mask: int32 [16, 128], P('dp'), may hold values 0 or 1
- lengths: int32 [16], P('dp'), may hold values from 16 to 128
- prompt_of: int32 [16], P('dp'), may hold values from 0 to 1, as said below
- old_logprob: float32 [16, 128], P('dp'), may hold values from -14 to -10
- ref_logprob: bfloat16 [16, 128], P(None, 'dp'), may hold values from -14 to -10
- advantages: float32 [16, 128], P('dp'), may hold values from -8 to 8
- returns: float32 [16, 128], P('dp'), may hold values from -6 to 6
- critic_hidden: bfloat16 [16, 128, 5120], P(None, 'dp', 'tensor'), may hold values from -6 to 6
- value_weight: bfloat16 [5120], P('tensor'), may hold values from -0.078125 to 0.078125
Outputs:
- token_loss: float32 [16, 128], P('dp')
- critic_grad: bfloat16 [16, 128, 5120], P(None, 'dp', 'tensor')
The draws below stay inside these ranges and needn't reach their ends.
Inputs may be any that keep to these rules, and one draw needn't show every extreme that they name: `prompt_of`: each of the 2 prompts is named by exactly 8 sequences.
All inputs are finite; a program needn't handle non-finite values. No bound on the sum of `response_mask` on one device may be relied on, other than what follows from the above.
Results may differ from the reference program's by a relative error of at most 0.001.
Values may be sent and summed in bfloat16 or wider, within the bound.
A program may use at most 64 MiB of HBM per device.

```python
import math
import jax
import jax.numpy as jnp
import numpy as np
from jax import lax

D = 5120
LEN = 128
RESPONSES = 8
BATCH = 16
VOCAB = 19456
PROMPTS = 2


def draw_logits(key, part):
    first_key = jax.random.fold_in(key, 0)
    full_shape = (BATCH, LEN, VOCAB)
    values = 1.5 * jax.random.truncated_normal(first_key, -6.0, 6.0, full_shape, jnp.float32)
    return values.astype(jnp.bfloat16)


def draw_prompt_of(key, part):
    order = jax.random.permutation(jax.random.fold_in(key, 7), BATCH)
    return (order // RESPONSES).astype(jnp.int32)


def plant(result, rng, least, high):
    longest = result.shape.index(max(result.shape))
    spots = []
    for shift in (0, 1):
        where = [jax.random.randint(jax.random.fold_in(rng, axis), (), 0, length) for axis, length in enumerate(result.shape)]
        where[longest] = (where[longest] + shift) % result.shape[longest]
        spots.append(tuple(where))
    return result.at[spots[0]].set(least).at[spots[1]].set(high)


def level_of(stream_key, shape, cuts, low, top_value):
    factor_of, own = 1.0, jax.random.fold_in(stream_key, 6)
    for dim, parts in cuts:
        steps = jnp.exp(jax.random.uniform(jax.random.fold_in(own, dim), (parts,), jnp.float32, low / len(cuts), top_value / len(cuts)))
        factor_of = factor_of * jnp.repeat(steps, shape[dim] // parts).reshape([-1 if axis == dim else 1 for axis in range(len(shape))])
    return factor_of


def rank_bounds(number_of, slope):
    weights = [(1 << 20) // math.isqrt(grade ** slope) + 1 for grade in range(1, number_of + 1)]
    spread = 1 + sum(weights) // (1 << 30)
    return np.cumsum(np.array([max(1, weight // spread) for weight in weights]))


def ranked(own_key, extent, count, slope):
    grid = rank_bounds(count, slope)
    lot = jax.random.randint(jax.random.fold_in(own_key, 1), extent, 0, int(grid[count - 1]))
    rank = jnp.searchsorted(jnp.asarray(grid, jnp.int32), lot, side="right")
    return jax.random.permutation(jax.random.fold_in(own_key, 2), count)[rank].astype(jnp.int32)


def gaussian(stream_key, shape, scale, most, pieces=(), kind=jnp.bfloat16):
    result = scale * jax.random.normal(stream_key, shape, jnp.float32)
    if pieces:
        result = result * level_of(stream_key, shape, pieces, -0.22, 0.18)
    return jnp.clip(result, -most, most).astype(kind)


def setup_inputs(seed: int = 0) -> dict:
    keys = jax.random.split(jax.random.key(seed), 12)
    return {
        "logits": draw_logits(jax.random.fold_in(keys[11], 71), 0),
        "token_ids": plant(ranked(keys[1], (BATCH, LEN), VOCAB, 2), jax.random.fold_in(keys[1], 3), 0, VOCAB - 1).astype(jnp.int32),
        "response_mask": plant((jax.random.randint(keys[2], (BATCH, LEN), 0, 8) < 7).astype(jnp.int32), jax.random.fold_in(keys[2], 1), 0, 1),
        "lengths": plant(jax.random.randint(keys[3], (BATCH,), LEN // 8, LEN + 1), jax.random.fold_in(keys[3], 1), LEN // 8, LEN).astype(jnp.int32),
        "prompt_of": draw_prompt_of(jax.random.fold_in(keys[11], 71), 0),
        "old_logprob": jnp.clip(-14.0 + 4.0 * jax.random.uniform(keys[5], (BATCH, LEN), jnp.float32) ** level_of(keys[5], (BATCH, LEN), ((0, 8),), -0.2, 0.2), -14.0, -10.0),
        "ref_logprob": jnp.clip(-14.0 + 4.0 * jax.random.uniform(keys[6], (BATCH, LEN), jnp.float32) ** level_of(keys[6], (BATCH, LEN), ((1, 8),), -0.2, 0.2), -14.0, -10.0).astype(jnp.bfloat16),
        "advantages": gaussian(keys[7], (BATCH, LEN), 2.0, 8.0, ((0, 8),), jnp.float32),
        "returns": gaussian(keys[8], (BATCH, LEN), 1.0, 6.0, ((0, 8),), jnp.float32),
        "critic_hidden": gaussian(keys[9], (BATCH, LEN, D), 1.0, 6.0, ((1, 8), (2, 4))),
        "value_weight": gaussian(keys[10], (D,), D ** -0.5, 0.078125, ((0, 4),)),
    }


def token_logprob(inputs):
    row_block, row_ids = inputs
    row_max = lax.optimization_barrier(jnp.max(row_block, axis=1)).astype(jnp.float32)
    exp_total = lax.optimization_barrier(jnp.sum(jnp.exp(row_block.astype(jnp.float32) - row_max[:, None]), axis=1))
    picked = jnp.take_along_axis(row_block, row_ids[:, None].astype(jnp.int32), axis=1)[:, 0].astype(jnp.float32)
    return picked - (row_max + jnp.log(exp_total))

def reference(logits, token_ids, response_mask, lengths, prompt_of, old_logprob, ref_logprob, advantages, returns, critic_hidden, value_weight):
    highest = lax.Precision.HIGHEST
    logprob = lax.map(token_logprob, (logits, token_ids))
    head_weight = value_weight.astype(jnp.float32)
    value_pred = jnp.einsum('bld,d->bl', critic_hidden.astype(jnp.float32), head_weight)
    position = jnp.arange(LEN, dtype=jnp.int32)
    live_mask = (response_mask * (position[None, :] < lengths[:, None]).astype(jnp.int32)).astype(jnp.float32)
    prompt_hot = (prompt_of[:, None] == jnp.arange(PROMPTS, dtype=jnp.int32)[None, :]).astype(jnp.float32)
    seq_tokens = lax.optimization_barrier(jnp.sum(live_mask, axis=1))
    seq_total = lax.optimization_barrier(jnp.sum(live_mask * advantages, axis=1))
    count_floor = jnp.maximum(jnp.dot(seq_tokens, prompt_hot, precision=highest), 1.0)
    prompt_mean = jnp.dot(seq_total, prompt_hot, precision=highest) / count_floor
    row_mean = jnp.dot(prompt_hot, prompt_mean, precision=highest)
    centered = advantages - row_mean[:, None]
    seq_square = lax.optimization_barrier(jnp.sum(live_mask * centered * centered, axis=1))
    prompt_var = jnp.dot(seq_square, prompt_hot, precision=highest) / count_floor
    row_scale = 1.0 / jnp.sqrt(jnp.dot(prompt_hot, prompt_var, precision=highest) + 1.0)
    whitened = centered * row_scale[:, None]
    prob_ratio = jnp.exp(jnp.clip(logprob - old_logprob, -20.0, 20.0))
    surrogate = jnp.maximum(-whitened * prob_ratio, -whitened * jnp.clip(prob_ratio, 0.8, 1.2))
    surrogate = jnp.where(whitened < 0.0, jnp.minimum(surrogate, -3.0 * whitened), surrogate)
    ref_drift = jnp.clip(ref_logprob.astype(jnp.float32) - logprob, -20.0, 20.0)
    penalty = jnp.clip(jnp.exp(ref_drift) - ref_drift - 1.0, -10.0, 10.0)
    value_error = value_pred - returns
    token_loss = live_mask * (surrogate + 0.1 * penalty + 0.25 * value_error * value_error)
    grad_coeff = 32.0 * live_mask * value_error
    critic_grad = (grad_coeff[:, :, None] * head_weight[None, None, :]).astype(jnp.bfloat16)
    return (token_loss, critic_grad)
```

```python
import functools

import jax
import jax.numpy as jnp
from jax import lax
from jax.experimental import pallas as pl
from jax.experimental.pallas import tpu as pltpu
from jax.sharding import PartitionSpec as P

F32 = jnp.float32
BF16 = jnp.bfloat16
MESH = pl.DeviceIdType.MESH
LANES = 128
ROWS = 32


def select_dot(x, hot):
    hi = x.astype(BF16)
    rest = x - hi.astype(F32)
    mid = rest.astype(BF16)
    low = (rest - mid.astype(F32)).astype(BF16)
    n = x.shape[0]
    out = jnp.dot(jnp.concatenate([hi, mid, low], axis=0), hot, preferred_element_type=F32)
    return out[:n] + out[n : 2 * n] + out[2 * n :]


def kernel(
    dims,
    logits_hbm, ids_hbm, mask_hbm, len_hbm, prompt_hbm, old_hbm, ref_hbm, adv_hbm, ret_hbm,
    hidden_hbm, weight_hbm,
    loss_ref, coeff_ref,
    logits, ids, mask, lens, prompts, old, ref, adv, ret, hidden, weight,
    top_col, sum_col, hit_col, id_col,
    early, value_part, stats, value_sum,
    in_sem, logit_sem,
    e_send, e_recv, v_send, v_recv, s_send, s_recv, w_send, w_recv,
):
    dp, tensor, seq_rows, seq_len, vocab, all_seqs, tile = dims
    wide = seq_rows * seq_len
    me_dp = lax.axis_index("dp")
    me_t = lax.axis_index("tensor")

    smalls = [
        pltpu.make_async_copy(src, dst, in_sem.at[n])
        for n, (src, dst) in enumerate(
            [
                (hidden_hbm, hidden), (weight_hbm, weight), (ids_hbm, ids), (mask_hbm, mask),
                (len_hbm, lens), (prompt_hbm, prompts), (ref_hbm, ref), (adv_hbm, adv),
                (ret_hbm, ret), (old_hbm, old),
            ]
        )
    ]
    bigs = [
        pltpu.make_async_copy(logits_hbm.at[r], logits.at[r], logit_sem.at[r])
        for r in range(seq_rows)
    ]
    barrier = pltpu.get_barrier_semaphore()
    for d in range(1, dp):
        pl.semaphore_signal(
            barrier, inc=1, device_id=(lax.rem(me_dp + d, dp), me_t), device_id_type=MESH
        )
    for d in range(1, tensor):
        pl.semaphore_signal(
            barrier, inc=1, device_id=(me_dp, lax.rem(me_t + d, tensor)), device_id_type=MESH
        )
    for c in smalls + bigs:
        c.start()

    def over_dp(buf, send, recv):
        return [
            pltpu.make_async_remote_copy(
                src_ref=buf.at[me_dp], dst_ref=buf.at[me_dp],
                send_sem=send.at[d - 1], recv_sem=recv.at[d - 1],
                device_id=(lax.rem(me_dp + d, dp), me_t), device_id_type=MESH,
            )
            for d in range(1, dp)
        ]

    def over_tensor(buf, send, recv):
        return [
            pltpu.make_async_remote_copy(
                src_ref=buf.at[me_t], dst_ref=buf.at[me_t],
                send_sem=send.at[d - 1], recv_sem=recv.at[d - 1],
                device_id=(me_dp, lax.rem(me_t + d, tensor)), device_id_type=MESH,
            )
            for d in range(1, tensor)
        ]

    e_copies = over_dp(early, e_send, e_recv)
    v_copies = over_tensor(value_part, v_send, v_recv)
    s_copies = over_tensor(stats, s_send, s_recv)
    w_copies = over_dp(value_sum, w_send, w_recv)

    smalls[0].wait()
    smalls[1].wait()
    head = jnp.broadcast_to(weight[...], (16, weight.shape[1]))
    part = lax.dot_general(
        head, hidden[...], (((1,), (1,)), ((), ())), preferred_element_type=F32
    )
    value_part[me_t] = part[:8]

    for c in smalls[2:]:
        c.wait()

    def flat(x):
        return jnp.concatenate([x[r : r + 1] for r in range(seq_rows)], axis=1)

    lane = lax.broadcasted_iota(jnp.int32, (1, wide), 1)
    seq_of = lane // seq_len
    len_row = jnp.zeros((1, wide), jnp.int32)
    prompt_row = jnp.zeros((1, wide), jnp.int32)
    for r in range(seq_rows):
        len_row = jnp.where(seq_of == r, lens[r], len_row)
        prompt_row = jnp.where(seq_of == r, prompts[r], prompt_row)
    live = (flat(mask[...]) * (lane % seq_len < len_row).astype(jnp.int32)).astype(F32)
    adv_row = flat(adv[...])
    ret_row = flat(ret[...])
    if tile % 16 == 0:
        spread = (
            lax.broadcasted_iota(jnp.int32, (tile, wide), 0)
            == lax.broadcasted_iota(jnp.int32, (tile, wide), 1) % tile
        ).astype(F32).astype(BF16)
        ref_wide = jnp.dot(ref[...], spread, preferred_element_type=F32)
        owner = (
            lax.broadcasted_iota(jnp.int32, (all_seqs, wide), 0)
            == lax.broadcasted_iota(jnp.int32, (all_seqs, wide), 1) // tile
        )
        ref_row = jnp.sum(jnp.where(owner, ref_wide, 0.0), axis=0, keepdims=True)
    else:
        ref_row = ref[...].astype(F32)
    early[me_dp] = jnp.concatenate(
        [ret_row, live, adv_row, prompt_row.astype(F32), ref_row, jnp.zeros((3, wide), F32)],
        axis=0,
    )

    start = me_t * vocab
    lane_block = lax.broadcasted_iota(jnp.int32, (ROWS, LANES), 1)

    def column(row):
        return jnp.broadcast_to(row, (LANES, LANES)).T

    def logit_pass(r):
        bigs[r].wait()
        for h in range(seq_len // LANES):
            id_row = (ids[r : r + 1, h * LANES : (h + 1) * LANES] - start).astype(F32)
            id_col[h * LANES : (h + 1) * LANES, :] = column(id_row).astype(jnp.int32)

        def top_step(n, _):
            rows = pl.ds(pl.multiple_of(n * ROWS, ROWS), ROWS)
            top = logits[r, rows, 0:LANES]
            for c in range(1, vocab // LANES):
                top = jnp.maximum(top, logits[r, rows, c * LANES : (c + 1) * LANES])
            peak = jnp.max(top.astype(F32), axis=1, keepdims=True)
            top_col[rows, :] = jnp.broadcast_to(peak, (ROWS, LANES))
            return 0

        lax.fori_loop(0, seq_len // ROWS, top_step, 0, unroll=True)

        def sum_step(n, _):
            rows = pl.ds(pl.multiple_of(n * ROWS, ROWS), ROWS)
            peak = top_col[rows, :]
            want = id_col[rows, :]
            total = jnp.zeros((ROWS, LANES), F32)
            hit = jnp.zeros((ROWS, LANES), F32)
            for c in range(vocab // LANES):
                x = logits[r, rows, c * LANES : (c + 1) * LANES].astype(F32)
                total = total + jnp.exp(x - peak)
                hit = jnp.where(lane_block + c * LANES == want, x, hit)
            sum_col[rows, :] = total
            hit_col[rows, :] = hit
            return 0

        lax.fori_loop(0, seq_len // ROWS, sum_step, 0)
        for h in range(seq_len // LANES):
            rows = slice(h * LANES, (h + 1) * LANES)
            cols = slice(r * seq_len + h * LANES, r * seq_len + (h + 1) * LANES)
            stats[me_t, 0:1, cols] = top_col[rows, :].T[0:1]
            stats[me_t, 1:2, cols] = jnp.sum(sum_col[rows, :].T, axis=0, keepdims=True)
            stats[me_t, 2:3, cols] = jnp.sum(hit_col[rows, :].T, axis=0, keepdims=True)

    stats[me_t, 3:8, :] = jnp.zeros((5, wide), F32)
    split = (seq_rows + 1) // 2
    for r in range(split):
        logit_pass(r)
    pl.semaphore_wait(barrier, dp - 1 + tensor - 1)
    for c in v_copies + e_copies:
        c.start()
    for r in range(split, seq_rows):
        logit_pass(r)
    for c in s_copies:
        c.start()

    for c in v_copies:
        c.wait_recv()
    value = value_part[0]
    for j in range(1, tensor):
        value = value + value_part[j]
    value_sum[me_dp] = value
    for c in w_copies:
        c.start()

    for c in e_copies:
        c.wait_recv()
    rows_all = early[...].reshape(dp * 8, wide)
    k = lax.broadcasted_iota(jnp.int32, (wide, wide), 0)
    l = lax.broadcasted_iota(jnp.int32, (wide, wide), 1)
    to_tile = (k == ((l // tile) % seq_rows) * seq_len + me_dp * tile + l % tile).astype(F32)
    to_seq = (k == (me_dp * seq_rows + l // seq_len) * tile + l % tile).astype(F32)
    to_seq = to_seq.astype(BF16)
    moved = select_dot(rows_all, to_tile.astype(BF16))
    row_id = lax.broadcasted_iota(jnp.int32, (dp * 8, wide), 0)
    lane_id = lax.broadcasted_iota(jnp.int32, (dp * 8, wide), 1)
    from_seq = lane_id // (tile * seq_rows) * 8

    def fold(x, keep):
        return jnp.sum(jnp.where(keep, x, 0.0), axis=0, keepdims=True)

    ret_tile = fold(moved, row_id == from_seq)
    live_tile = fold(moved, row_id == from_seq + 1)
    coeff = 32.0 * live_tile * (value[0:1] - ret_tile)
    for h in range(wide // LANES):
        coeff_ref[h * LANES : (h + 1) * LANES, :] = column(coeff[:, h * LANES : (h + 1) * LANES])
    from_tile = (lane_id % seq_len) // tile * 8
    ref_seq = fold(select_dot(rows_all, to_seq), row_id == from_tile + 4)

    live_all = early[:, 1, :]
    adv_all = early[:, 2, :]
    prompt_all = early[:, 3, :]
    whitened = jnp.zeros((1, wide), F32)
    for r in range(seq_rows):
        same = jnp.where(prompt_all == prompts[r].astype(F32), live_all, 0.0)
        count = jnp.maximum(jnp.sum(same, keepdims=True), 1.0)
        mean = jnp.sum(same * adv_all, keepdims=True) / count
        off = adv_all - mean
        var = jnp.sum(same * off * off, keepdims=True) / count
        whitened = jnp.where(seq_of == r, (adv_row - mean) * lax.rsqrt(var + 1.0), whitened)

    for c in s_copies:
        c.wait_recv()
    row_max = stats[0, 0:1]
    for j in range(1, tensor):
        row_max = jnp.maximum(row_max, stats[j, 0:1])
    total = jnp.zeros((1, wide), F32)
    target = jnp.zeros((1, wide), F32)
    for j in range(tensor):
        total = total + stats[j, 1:2] * jnp.exp(stats[j, 0:1] - row_max)
        target = target + stats[j, 2:3]
    logprob = target - (row_max + jnp.log(total))
    prob_ratio = jnp.exp(jnp.clip(logprob - flat(old[...]), -20.0, 20.0))
    surrogate = jnp.maximum(-whitened * prob_ratio, -whitened * jnp.clip(prob_ratio, 0.8, 1.2))
    surrogate = jnp.where(whitened < 0.0, jnp.minimum(surrogate, -3.0 * whitened), surrogate)
    drift = jnp.clip(ref_seq - logprob, -20.0, 20.0)
    penalty = jnp.clip(jnp.exp(drift) - drift - 1.0, -10.0, 10.0)
    policy = surrogate + 0.1 * penalty

    for c in w_copies:
        c.wait_recv()
    value_rows = value_sum[...].reshape(dp * 8, wide)
    value_seq = fold(select_dot(value_rows, to_seq), row_id == from_tile)
    error = value_seq - ret_row
    loss = live * (policy + 0.25 * error * error)
    for r in range(seq_rows):
        loss_ref[r : r + 1, :] = loss[:, r * seq_len : (r + 1) * seq_len]
    for c in v_copies + e_copies + s_copies + w_copies:
        c.wait_send()


def per_device(
    logits, token_ids, response_mask, lengths, prompt_of, old_logprob, ref_logprob, advantages,
    returns, critic_hidden, value_weight,
):
    seq_rows, seq_len, vocab = logits.shape
    all_seqs, tile, feats = critic_hidden.shape
    dp = lax.axis_size("dp")
    tensor = lax.axis_size("tensor")
    wide = seq_rows * seq_len
    ref = ref_logprob if tile % 16 == 0 else ref_logprob.reshape(1, wide)
    args = (
        logits, token_ids, response_mask, lengths, prompt_of, old_logprob, ref, advantages,
        returns, critic_hidden.reshape(all_seqs * tile, feats), value_weight.reshape(1, feats),
    )
    scratch = [
        pltpu.SMEM(x.shape, x.dtype) if x.ndim == 1 else pltpu.VMEM(x.shape, x.dtype)
        for x in args
    ]
    scratch += [pltpu.VMEM((seq_len, LANES), t) for t in (F32, F32, F32, jnp.int32)]
    scratch += [pltpu.VMEM((n, 8, wide), F32) for n in (dp, tensor, tensor, dp)]
    dma = pltpu.SemaphoreType.DMA
    scratch += [dma((10,)), dma((seq_rows,))]
    for n in (dp, tensor, tensor, dp):
        scratch += [dma((n - 1,)), dma((n - 1,))]
    dims = (dp, tensor, seq_rows, seq_len, vocab, all_seqs, tile)
    token_loss, coeff = pl.pallas_call(
        functools.partial(kernel, dims),
        out_shape=(
            jax.ShapeDtypeStruct((seq_rows, seq_len), F32),
            jax.ShapeDtypeStruct((wide, LANES), F32),
        ),
        in_specs=[pl.BlockSpec(memory_space=pl.ANY)] * len(args),
        out_specs=(pl.BlockSpec(memory_space=pltpu.VMEM), pl.BlockSpec(memory_space=pltpu.VMEM)),
        scratch_shapes=scratch,
        compiler_params=pltpu.CompilerParams(collective_id=0, has_side_effects=True),
        name="ppo",
    )(*args)
    grad = (coeff[:, 0:1] * value_weight.astype(F32)[None, :]).astype(BF16)
    return token_loss, grad.reshape(all_seqs, tile, feats)


def solution(mesh):
    in_specs = (
        P("dp", None, "tensor"),
        P("dp", None),
        P("dp", None),
        P("dp"),
        P("dp"),
        P("dp", None),
        P(None, "dp"),
        P("dp", None),
        P("dp", None),
        P(None, "dp", "tensor"),
        P("tensor"),
    )
    out_specs = (P("dp", None), P(None, "dp", "tensor"))
    return jax.shard_map(
        per_device, mesh=mesh, in_specs=in_specs, out_specs=out_specs, check_vma=False
    )
```

```python
import functools

import jax
import jax.numpy as jnp
from jax import lax
from jax.experimental import pallas as pl
from jax.experimental.pallas import tpu as pltpu
from jax.sharding import PartitionSpec as P

F32 = jnp.float32
BF16 = jnp.bfloat16
MESH = pl.DeviceIdType.MESH
LANES = 128
ROWS = 32
PIECES = 4


def select_dot(x, hot):
    hi = x.astype(BF16)
    rest = x - hi.astype(F32)
    mid = rest.astype(BF16)
    low = (rest - mid.astype(F32)).astype(BF16)
    n = x.shape[0]
    out = jnp.dot(jnp.concatenate([hi, mid, low], axis=0), hot, preferred_element_type=F32)
    return out[:n] + out[n : 2 * n] + out[2 * n :]


def kernel(
    dims,
    logits_hbm, ids_hbm, mask_hbm, len_hbm, prompt_hbm, old_hbm, ref_hbm, adv_hbm, ret_hbm,
    hidden_hbm, weight_hbm,
    loss_ref, grad_ref,
    logits, ids, mask, lens, prompts, old, ref, adv, ret, hidden, weight,
    top_col, sum_col, hit_col, id_col,
    early, value_part, stats, value_sum,
    in_sem, logit_sem,
    e_send, e_recv, v_send, v_recv, s_send, s_recv, w_send, w_recv,
):
    dp, tensor, seq_rows, seq_len, vocab, all_seqs, tile = dims
    wide = seq_rows * seq_len
    me_dp = lax.axis_index("dp")
    me_t = lax.axis_index("tensor")

    smalls = [
        pltpu.make_async_copy(src, dst, in_sem.at[n])
        for n, (src, dst) in enumerate(
            [
                (hidden_hbm, hidden), (weight_hbm, weight), (ids_hbm, ids), (mask_hbm, mask),
                (len_hbm, lens), (prompt_hbm, prompts), (ref_hbm, ref), (adv_hbm, adv),
                (ret_hbm, ret), (old_hbm, old),
            ]
        )
    ]
    bigs = [
        pltpu.make_async_copy(logits_hbm.at[r], logits.at[r], logit_sem.at[r])
        for r in range(seq_rows)
    ]
    barrier = pltpu.get_barrier_semaphore()
    for d in range(1, dp):
        pl.semaphore_signal(
            barrier, inc=1, device_id=(lax.rem(me_dp + d, dp), me_t), device_id_type=MESH
        )
    for d in range(1, tensor):
        pl.semaphore_signal(
            barrier, inc=1, device_id=(me_dp, lax.rem(me_t + d, tensor)), device_id_type=MESH
        )
    for c in smalls + bigs:
        c.start()

    def over_dp(buf, send, recv):
        return [
            pltpu.make_async_remote_copy(
                src_ref=buf.at[me_dp], dst_ref=buf.at[me_dp],
                send_sem=send.at[d - 1], recv_sem=recv.at[d - 1],
                device_id=(lax.rem(me_dp + d, dp), me_t), device_id_type=MESH,
            )
            for d in range(1, dp)
        ]

    def over_tensor(buf, send, recv):
        return [
            pltpu.make_async_remote_copy(
                src_ref=buf.at[me_t], dst_ref=buf.at[me_t],
                send_sem=send.at[d - 1], recv_sem=recv.at[d - 1],
                device_id=(me_dp, lax.rem(me_t + d, tensor)), device_id_type=MESH,
            )
            for d in range(1, tensor)
        ]

    e_copies = over_dp(early, e_send, e_recv)
    v_copies = over_tensor(value_part, v_send, v_recv)
    s_copies = over_tensor(stats, s_send, s_recv)
    w_copies = over_dp(value_sum, w_send, w_recv)

    smalls[0].wait()
    smalls[1].wait()
    head_row = weight[...].reshape(1, weight.shape[0])
    head = jnp.broadcast_to(head_row, (16, weight.shape[0]))
    part = lax.dot_general(
        head, hidden[...], (((1,), (1,)), ((), ())), preferred_element_type=F32
    )
    value_part[me_t] = part[:8]
    pl.semaphore_wait(barrier, dp - 1 + tensor - 1)
    for c in v_copies:
        c.start()

    for c in smalls[2:]:
        c.wait()

    def flat(x):
        return jnp.concatenate([x[r : r + 1] for r in range(seq_rows)], axis=1)

    lane = lax.broadcasted_iota(jnp.int32, (1, wide), 1)
    seq_of = lane // seq_len
    len_row = jnp.zeros((1, wide), jnp.int32)
    prompt_row = jnp.zeros((1, wide), jnp.int32)
    for r in range(seq_rows):
        len_row = jnp.where(seq_of == r, lens[r], len_row)
        prompt_row = jnp.where(seq_of == r, prompts[r], prompt_row)
    live = (flat(mask[...]) * (lane % seq_len < len_row).astype(jnp.int32)).astype(F32)
    adv_row = flat(adv[...])
    ret_row = flat(ret[...])
    if tile % 16 == 0:
        spread = (
            lax.broadcasted_iota(jnp.int32, (tile, wide), 0)
            == lax.broadcasted_iota(jnp.int32, (tile, wide), 1) % tile
        ).astype(F32).astype(BF16)
        ref_wide = jnp.dot(ref[...], spread, preferred_element_type=F32)
        owner = (
            lax.broadcasted_iota(jnp.int32, (all_seqs, wide), 0)
            == lax.broadcasted_iota(jnp.int32, (all_seqs, wide), 1) // tile
        )
        ref_row = jnp.sum(jnp.where(owner, ref_wide, 0.0), axis=0, keepdims=True)
    else:
        ref_row = ref[...].astype(F32)
    early[me_dp] = jnp.concatenate(
        [ret_row, live, adv_row, prompt_row.astype(F32), ref_row, jnp.zeros((3, wide), F32)],
        axis=0,
    )
    for c in e_copies:
        c.start()

    start = me_t * vocab
    lane_block = lax.broadcasted_iota(jnp.int32, (ROWS, LANES), 1)

    def column(row):
        return jnp.broadcast_to(row, (LANES, LANES)).T

    def logit_pass(r):
        bigs[r].wait()
        for h in range(seq_len // LANES):
            id_row = (ids[r : r + 1, h * LANES : (h + 1) * LANES] - start).astype(F32)
            id_col[h * LANES : (h + 1) * LANES, :] = column(id_row).astype(jnp.int32)

        def top_step(n, _):
            rows = pl.ds(pl.multiple_of(n * ROWS, ROWS), ROWS)
            top = logits[r, rows, 0:LANES]
            for c in range(1, vocab // LANES):
                top = jnp.maximum(top, logits[r, rows, c * LANES : (c + 1) * LANES])
            peak = jnp.max(top.astype(F32), axis=1, keepdims=True)
            top_col[rows, :] = jnp.broadcast_to(peak, (ROWS, LANES))
            return 0

        lax.fori_loop(0, seq_len // ROWS, top_step, 0, unroll=True)

        def sum_step(n, _):
            rows = pl.ds(pl.multiple_of(n * ROWS, ROWS), ROWS)
            peak = top_col[rows, :]
            want = id_col[rows, :]
            total = jnp.zeros((ROWS, LANES), F32)
            hit = jnp.zeros((ROWS, LANES), F32)
            for c in range(vocab // LANES):
                x = logits[r, rows, c * LANES : (c + 1) * LANES].astype(F32)
                total = total + jnp.exp(x - peak)
                hit = jnp.where(lane_block + c * LANES == want, x, hit)
            sum_col[rows, :] = total
            hit_col[rows, :] = hit
            return 0

        lax.fori_loop(0, seq_len // ROWS, sum_step, 0)
        for h in range(seq_len // LANES):
            rows = slice(h * LANES, (h + 1) * LANES)
            cols = slice(r * seq_len + h * LANES, r * seq_len + (h + 1) * LANES)
            stats[me_t, 0:1, cols] = top_col[rows, :].T[0:1]
            stats[me_t, 1:2, cols] = jnp.sum(sum_col[rows, :].T, axis=0, keepdims=True)
            stats[me_t, 2:3, cols] = jnp.sum(hit_col[rows, :].T, axis=0, keepdims=True)

    stats[me_t, 3:8, :] = jnp.zeros((5, wide), F32)
    split = (seq_rows + 1) // 2
    for r in range(split):
        logit_pass(r)

    for c in v_copies:
        c.wait_recv()
    value = value_part[0]
    for j in range(1, tensor):
        value = value + value_part[j]
    value_sum[me_dp] = value
    for c in w_copies:
        c.start()

    for r in range(split, seq_rows):
        logit_pass(r)
    for c in s_copies:
        c.start()

    for c in e_copies:
        c.wait_recv()
    k = lax.broadcasted_iota(jnp.int32, (wide, wide), 0)
    l = lax.broadcasted_iota(jnp.int32, (wide, wide), 1)
    to_tile = (k == ((l // tile) % seq_rows) * seq_len + me_dp * tile + l % tile).astype(F32)
    to_seq = (k == (me_dp * seq_rows + l // seq_len) * tile + l % tile).astype(F32)
    to_seq = to_seq.astype(BF16)
    row_id = lax.broadcasted_iota(jnp.int32, (dp, wide), 0)
    lane_id = lax.broadcasted_iota(jnp.int32, (dp, wide), 1)
    from_seq = row_id == lane_id // (tile * seq_rows)
    from_tile = row_id == (lane_id % seq_len) // tile

    def fold(x, keep):
        return jnp.sum(jnp.where(keep, x, 0.0), axis=0, keepdims=True)

    moved = select_dot(
        jnp.concatenate([early[:, 0, :], early[:, 1, :]], axis=0), to_tile.astype(BF16)
    )
    ret_tile = fold(moved[:dp], from_seq)
    live_tile = fold(moved[dp:], from_seq)
    ref_seq = fold(
        jnp.dot(early[:, 4, :].astype(BF16), to_seq, preferred_element_type=F32), from_tile
    )

    coeff = 32.0 * live_tile * (value[0:1] - ret_tile)
    head32 = head_row.astype(F32)
    for h in range(wide // LANES):
        factor = column(coeff[:, h * LANES : (h + 1) * LANES])
        for c in range(head32.shape[1] // LANES):
            cols = slice(c * LANES, (c + 1) * LANES)
            grad_ref[h * LANES : (h + 1) * LANES, cols] = (factor * head32[:, cols]).astype(BF16)

    live_all = early[:, 1, :]
    adv_all = early[:, 2, :]
    prompt_all = early[:, 3, :]
    whitened = jnp.zeros((1, wide), F32)
    for r in range(seq_rows):
        same = jnp.where(prompt_all == prompts[r].astype(F32), live_all, 0.0)
        count = jnp.maximum(jnp.sum(same, keepdims=True), 1.0)
        mean = jnp.sum(same * adv_all, keepdims=True) / count
        off = adv_all - mean
        var = jnp.sum(same * off * off, keepdims=True) / count
        whitened = jnp.where(seq_of == r, (adv_row - mean) * lax.rsqrt(var + 1.0), whitened)

    for c in s_copies:
        c.wait_recv()
    row_max = stats[0, 0:1]
    for j in range(1, tensor):
        row_max = jnp.maximum(row_max, stats[j, 0:1])
    total = jnp.zeros((1, wide), F32)
    target = jnp.zeros((1, wide), F32)
    for j in range(tensor):
        total = total + stats[j, 1:2] * jnp.exp(stats[j, 0:1] - row_max)
        target = target + stats[j, 2:3]
    logprob = target - (row_max + jnp.log(total))
    prob_ratio = jnp.exp(jnp.clip(logprob - flat(old[...]), -20.0, 20.0))
    surrogate = jnp.maximum(-whitened * prob_ratio, -whitened * jnp.clip(prob_ratio, 0.8, 1.2))
    surrogate = jnp.where(whitened < 0.0, jnp.minimum(surrogate, -3.0 * whitened), surrogate)
    drift = jnp.clip(ref_seq - logprob, -20.0, 20.0)
    penalty = jnp.clip(jnp.exp(drift) - drift - 1.0, -10.0, 10.0)
    policy = surrogate + 0.1 * penalty

    for c in w_copies:
        c.wait_recv()
    value_seq = fold(select_dot(value_sum[:, 0, :], to_seq), from_tile)
    error = value_seq - ret_row
    loss = live * (policy + 0.25 * error * error)
    for r in range(seq_rows):
        loss_ref[r : r + 1, :] = loss[:, r * seq_len : (r + 1) * seq_len]
    for c in v_copies + e_copies + s_copies + w_copies:
        c.wait_send()


def write_out(loss_in, grad_in, loss_ref, grad_ref, sems):
    copies = [pltpu.make_async_copy(loss_in, loss_ref, sems.at[0])]
    step = grad_in.shape[0] // PIECES
    for n in range(PIECES):
        rows = pl.ds(n * step, step)
        copies.append(
            pltpu.make_async_copy(grad_in.at[rows], grad_ref.at[rows], sems.at[n + 1])
        )
    for c in copies:
        c.start()
    for c in copies:
        c.wait()


def per_device(
    logits, token_ids, response_mask, lengths, prompt_of, old_logprob, ref_logprob, advantages,
    returns, critic_hidden, value_weight,
):
    seq_rows, seq_len, vocab = logits.shape
    all_seqs, tile, feats = critic_hidden.shape
    dp = lax.axis_size("dp")
    tensor = lax.axis_size("tensor")
    wide = seq_rows * seq_len
    ref = ref_logprob if tile % 16 == 0 else ref_logprob.reshape(1, wide)
    args = (
        logits, token_ids, response_mask, lengths, prompt_of, old_logprob, ref, advantages,
        returns, critic_hidden.reshape(all_seqs * tile, feats), value_weight,
    )
    args = tuple(pltpu.with_memory_space_constraint(x, pltpu.HBM) for x in args)
    scratch = [
        pltpu.SMEM(x.shape, x.dtype) if x.shape == (seq_rows,) else pltpu.VMEM(x.shape, x.dtype)
        for x in args
    ]
    scratch += [pltpu.VMEM((seq_len, LANES), t) for t in (F32, F32, F32, jnp.int32)]
    scratch += [pltpu.VMEM((n, 8, wide), F32) for n in (dp, tensor, tensor, dp)]
    dma = pltpu.SemaphoreType.DMA
    scratch += [dma((10,)), dma((seq_rows,))]
    for n in (dp, tensor, tensor, dp):
        scratch += [dma((n - 1,)), dma((n - 1,))]
    dims = (dp, tensor, seq_rows, seq_len, vocab, all_seqs, tile)
    token_loss, grad = pl.pallas_call(
        functools.partial(kernel, dims),
        out_shape=(
            jax.ShapeDtypeStruct((seq_rows, seq_len), F32),
            jax.ShapeDtypeStruct((wide, feats), BF16),
        ),
        in_specs=[pl.BlockSpec(memory_space=pltpu.HBM)] * len(args),
        out_specs=(pl.BlockSpec(memory_space=pltpu.VMEM), pl.BlockSpec(memory_space=pltpu.VMEM)),
        scratch_shapes=scratch,
        compiler_params=pltpu.CompilerParams(
            collective_id=0, has_side_effects=True, vmem_limit_bytes=16 << 20
        ),
        name="ppo",
    )(*args)
    token_loss, grad = pl.pallas_call(
        write_out,
        out_shape=(
            jax.ShapeDtypeStruct((seq_rows, seq_len), F32),
            jax.ShapeDtypeStruct((wide, feats), BF16),
        ),
        in_specs=[pl.BlockSpec(memory_space=pltpu.VMEM)] * 2,
        out_specs=(pl.BlockSpec(memory_space=pltpu.HBM),) * 2,
        scratch_shapes=[dma((PIECES + 1,))],
        compiler_params=pltpu.CompilerParams(vmem_limit_bytes=16 << 20),
        name="tail",
    )(token_loss, grad)
    return token_loss, grad.reshape(all_seqs, tile, feats)


def solution(mesh):
    in_specs = (
        P("dp", None, "tensor"),
        P("dp", None),
        P("dp", None),
        P("dp"),
        P("dp"),
        P("dp", None),
        P(None, "dp"),
        P("dp", None),
        P("dp", None),
        P(None, "dp", "tensor"),
        P("tensor"),
    )
    out_specs = (P("dp", None), P(None, "dp", "tensor"))
    return jax.shard_map(
        per_device, mesh=mesh, in_specs=in_specs, out_specs=out_specs, check_vma=False
    )
```

```python
import functools

import jax
import jax.numpy as jnp
from jax import lax
from jax.experimental import pallas as pl
from jax.experimental.pallas import tpu as pltpu
from jax.sharding import PartitionSpec as P

F32 = jnp.float32
BF16 = jnp.bfloat16
MESH = pl.DeviceIdType.MESH
LANES = 128
ROWS = 32
PIECES = 4


def select_dot(x, hot):
    hi = x.astype(BF16)
    rest = x - hi.astype(F32)
    mid = rest.astype(BF16)
    low = (rest - mid.astype(F32)).astype(BF16)
    n = x.shape[0]
    out = jnp.dot(jnp.concatenate([hi, mid, low], axis=0), hot, preferred_element_type=F32)
    return out[:n] + out[n : 2 * n] + out[2 * n :]


def kernel(
    dims,
    logits_hbm, ids_hbm, mask_hbm, len_hbm, prompt_hbm, old_hbm, ref_hbm, adv_hbm, ret_hbm,
    hidden_hbm, weight_hbm,
    loss_ref, grad_ref,
    logits, ids, mask, lens, prompts, old, ref, adv, ret, hidden, weight,
    top_col, sum_col, hit_col, id_col,
    early, value_part, stats, value_sum,
    in_sem, logit_sem,
    e_send, e_recv, v_send, v_recv, s_send, s_recv, w_send, w_recv,
):
    dp, tensor, seq_rows, seq_len, vocab, all_seqs, tile = dims
    wide = seq_rows * seq_len
    me_dp = lax.axis_index("dp")
    me_t = lax.axis_index("tensor")

    smalls = [
        pltpu.make_async_copy(src, dst, in_sem.at[n])
        for n, (src, dst) in enumerate(
            [
                (hidden_hbm, hidden), (weight_hbm, weight), (ids_hbm, ids), (mask_hbm, mask),
                (len_hbm, lens), (prompt_hbm, prompts), (ref_hbm, ref), (adv_hbm, adv),
                (ret_hbm, ret), (old_hbm, old),
            ]
        )
    ]
    bigs = [
        pltpu.make_async_copy(logits_hbm.at[r], logits.at[r], logit_sem.at[r])
        for r in range(seq_rows)
    ]
    barrier = pltpu.get_barrier_semaphore()
    for d in range(1, dp):
        pl.semaphore_signal(
            barrier, inc=1, device_id=(lax.rem(me_dp + d, dp), me_t), device_id_type=MESH
        )
    for d in range(1, tensor):
        pl.semaphore_signal(
            barrier, inc=1, device_id=(me_dp, lax.rem(me_t + d, tensor)), device_id_type=MESH
        )
    for c in smalls + bigs:
        c.start()

    def over_dp(buf, send, recv):
        return [
            pltpu.make_async_remote_copy(
                src_ref=buf.at[me_dp], dst_ref=buf.at[me_dp],
                send_sem=send.at[d - 1], recv_sem=recv.at[d - 1],
                device_id=(lax.rem(me_dp + d, dp), me_t), device_id_type=MESH,
            )
            for d in range(1, dp)
        ]

    def over_tensor(buf, send, recv):
        return [
            pltpu.make_async_remote_copy(
                src_ref=buf.at[me_t], dst_ref=buf.at[me_t],
                send_sem=send.at[d - 1], recv_sem=recv.at[d - 1],
                device_id=(me_dp, lax.rem(me_t + d, tensor)), device_id_type=MESH,
            )
            for d in range(1, tensor)
        ]

    e_copies = over_dp(early, e_send, e_recv)
    v_copies = over_tensor(value_part, v_send, v_recv)
    s_copies = over_tensor(stats, s_send, s_recv)
    w_copies = over_dp(value_sum, w_send, w_recv)

    smalls[0].wait()
    smalls[1].wait()
    head_row = weight[...].reshape(1, weight.shape[0])
    head = jnp.broadcast_to(head_row, (16, weight.shape[0]))
    part = lax.dot_general(
        head, hidden[...], (((1,), (1,)), ((), ())), preferred_element_type=F32
    )
    value_part[me_t] = part[:1]

    for c in smalls[2:]:
        c.wait()

    def flat(x):
        return jnp.concatenate([x[r : r + 1] for r in range(seq_rows)], axis=1)

    lane = lax.broadcasted_iota(jnp.int32, (1, wide), 1)
    seq_of = lane // seq_len
    len_row = jnp.zeros((1, wide), jnp.int32)
    prompt_row = jnp.zeros((1, wide), jnp.int32)
    for r in range(seq_rows):
        len_row = jnp.where(seq_of == r, lens[r], len_row)
        prompt_row = jnp.where(seq_of == r, prompts[r], prompt_row)
    live = (flat(mask[...]) * (lane % seq_len < len_row).astype(jnp.int32)).astype(F32)
    adv_row = flat(adv[...])
    ret_row = flat(ret[...])
    if tile % 16 == 0:
        spread = (
            lax.broadcasted_iota(jnp.int32, (tile, wide), 0)
            == lax.broadcasted_iota(jnp.int32, (tile, wide), 1) % tile
        ).astype(F32).astype(BF16)
        ref_wide = jnp.dot(ref[...], spread, preferred_element_type=F32)
        owner = (
            lax.broadcasted_iota(jnp.int32, (all_seqs, wide), 0)
            == lax.broadcasted_iota(jnp.int32, (all_seqs, wide), 1) // tile
        )
        ref_row = jnp.sum(jnp.where(owner, ref_wide, 0.0), axis=0, keepdims=True)
    else:
        ref_row = ref[...].astype(F32)
    code = live * (prompt_row.astype(F32) + 1.0)
    early[me_dp] = jnp.concatenate([ret_row, code, adv_row, ref_row], axis=0)

    start = me_t * vocab
    lane_block = lax.broadcasted_iota(jnp.int32, (ROWS, LANES), 1)

    def column(row):
        return jnp.broadcast_to(row, (LANES, LANES)).T

    def logit_pass(r):
        bigs[r].wait()
        for h in range(seq_len // LANES):
            id_row = (ids[r : r + 1, h * LANES : (h + 1) * LANES] - start).astype(F32)
            id_col[h * LANES : (h + 1) * LANES, :] = column(id_row).astype(jnp.int32)

        def top_step(n, _):
            rows = pl.ds(pl.multiple_of(n * ROWS, ROWS), ROWS)
            top = logits[r, rows, 0:LANES]
            for c in range(1, vocab // LANES):
                top = jnp.maximum(top, logits[r, rows, c * LANES : (c + 1) * LANES])
            peak = jnp.max(top.astype(F32), axis=1, keepdims=True)
            top_col[rows, :] = jnp.broadcast_to(peak, (ROWS, LANES))
            return 0

        lax.fori_loop(0, seq_len // ROWS, top_step, 0, unroll=True)

        def sum_step(n, _):
            rows = pl.ds(pl.multiple_of(n * ROWS, ROWS), ROWS)
            peak = top_col[rows, :]
            want = id_col[rows, :]
            total = jnp.zeros((ROWS, LANES), F32)
            hit = jnp.zeros((ROWS, LANES), F32)
            for c in range(vocab // LANES):
                x = logits[r, rows, c * LANES : (c + 1) * LANES].astype(F32)
                total = total + jnp.exp(x - peak)
                hit = jnp.where(lane_block + c * LANES == want, x, hit)
            sum_col[rows, :] = total
            hit_col[rows, :] = hit
            return 0

        lax.fori_loop(0, seq_len // ROWS, sum_step, 0)
        for h in range(seq_len // LANES):
            rows = slice(h * LANES, (h + 1) * LANES)
            cols = slice(r * seq_len + h * LANES, r * seq_len + (h + 1) * LANES)
            stats[me_t, 0:1, cols] = top_col[rows, :].T[0:1]
            stats[me_t, 1:2, cols] = jnp.sum(sum_col[rows, :].T, axis=0, keepdims=True)
            stats[me_t, 2:3, cols] = jnp.sum(hit_col[rows, :].T, axis=0, keepdims=True)

    stats[me_t, 3:4, :] = jnp.zeros((1, wide), F32)
    split = (seq_rows + 1) // 2
    for r in range(split):
        logit_pass(r)
    pl.semaphore_wait(barrier, dp - 1 + tensor - 1)
    for c in v_copies + e_copies:
        c.start()
    for r in range(split, seq_rows):
        logit_pass(r)
    for c in s_copies:
        c.start()

    for c in v_copies:
        c.wait_recv()
    value = value_part[0]
    for j in range(1, tensor):
        value = value + value_part[j]
    value_sum[me_dp] = value
    for c in w_copies:
        c.start()

    for c in e_copies:
        c.wait_recv()
    k = lax.broadcasted_iota(jnp.int32, (wide, wide), 0)
    l = lax.broadcasted_iota(jnp.int32, (wide, wide), 1)
    to_tile = (k == ((l // tile) % seq_rows) * seq_len + me_dp * tile + l % tile).astype(F32)
    to_seq = (k == (me_dp * seq_rows + l // seq_len) * tile + l % tile).astype(F32)
    to_seq = to_seq.astype(BF16)
    row_id = lax.broadcasted_iota(jnp.int32, (dp, wide), 0)
    lane_id = lax.broadcasted_iota(jnp.int32, (dp, wide), 1)
    from_seq = row_id == lane_id // (tile * seq_rows)
    from_tile = row_id == (lane_id % seq_len) // tile

    def fold(x, keep):
        return jnp.sum(jnp.where(keep, x, 0.0), axis=0, keepdims=True)

    code_all = early[:, 1, :]
    live_all = jnp.where(code_all > 0.0, 1.0, 0.0)
    moved = select_dot(
        jnp.concatenate([early[:, 0, :], live_all], axis=0), to_tile.astype(BF16)
    )
    ret_tile = fold(moved[:dp], from_seq)
    live_tile = fold(moved[dp:], from_seq)
    ref_seq = fold(
        jnp.dot(early[:, 3, :].astype(BF16), to_seq, preferred_element_type=F32), from_tile
    )

    coeff = 32.0 * live_tile * (value - ret_tile)
    head32 = head_row.astype(F32)
    for h in range(wide // LANES):
        factor = column(coeff[:, h * LANES : (h + 1) * LANES])
        for c in range(head32.shape[1] // LANES):
            cols = slice(c * LANES, (c + 1) * LANES)
            grad_ref[h * LANES : (h + 1) * LANES, cols] = (factor * head32[:, cols]).astype(BF16)

    adv_all = early[:, 2, :]
    whitened = jnp.zeros((1, wide), F32)
    for r in range(seq_rows):
        same = jnp.where(code_all == prompts[r].astype(F32) + 1.0, 1.0, 0.0)
        count = jnp.maximum(jnp.sum(same, keepdims=True), 1.0)
        mean = jnp.sum(same * adv_all, keepdims=True) / count
        off = adv_all - mean
        var = jnp.sum(same * off * off, keepdims=True) / count
        whitened = jnp.where(seq_of == r, (adv_row - mean) * lax.rsqrt(var + 1.0), whitened)

    for c in s_copies:
        c.wait_recv()
    row_max = stats[0, 0:1]
    for j in range(1, tensor):
        row_max = jnp.maximum(row_max, stats[j, 0:1])
    total = jnp.zeros((1, wide), F32)
    target = jnp.zeros((1, wide), F32)
    for j in range(tensor):
        total = total + stats[j, 1:2] * jnp.exp(stats[j, 0:1] - row_max)
        target = target + stats[j, 2:3]
    logprob = target - (row_max + jnp.log(total))
    prob_ratio = jnp.exp(jnp.clip(logprob - flat(old[...]), -20.0, 20.0))
    surrogate = jnp.maximum(-whitened * prob_ratio, -whitened * jnp.clip(prob_ratio, 0.8, 1.2))
    surrogate = jnp.where(whitened < 0.0, jnp.minimum(surrogate, -3.0 * whitened), surrogate)
    drift = jnp.clip(ref_seq - logprob, -20.0, 20.0)
    penalty = jnp.clip(jnp.exp(drift) - drift - 1.0, -10.0, 10.0)
    policy = surrogate + 0.1 * penalty

    for c in w_copies:
        c.wait_recv()
    value_seq = fold(select_dot(value_sum[:, 0, :], to_seq), from_tile)
    error = value_seq - ret_row
    loss = live * (policy + 0.25 * error * error)
    for r in range(seq_rows):
        loss_ref[r : r + 1, :] = loss[:, r * seq_len : (r + 1) * seq_len]
    for c in v_copies + e_copies + s_copies + w_copies:
        c.wait_send()


def write_out(loss_in, grad_in, loss_ref, grad_ref, sems):
    copies = [pltpu.make_async_copy(loss_in, loss_ref, sems.at[0])]
    step = grad_in.shape[0] // PIECES
    for n in range(PIECES):
        rows = pl.ds(n * step, step)
        copies.append(
            pltpu.make_async_copy(grad_in.at[rows], grad_ref.at[rows], sems.at[n + 1])
        )
    for c in copies:
        c.start()
    for c in copies:
        c.wait()


def per_device(
    logits, token_ids, response_mask, lengths, prompt_of, old_logprob, ref_logprob, advantages,
    returns, critic_hidden, value_weight,
):
    seq_rows, seq_len, vocab = logits.shape
    all_seqs, tile, feats = critic_hidden.shape
    dp = lax.axis_size("dp")
    tensor = lax.axis_size("tensor")
    wide = seq_rows * seq_len
    ref = ref_logprob if tile % 16 == 0 else ref_logprob.reshape(1, wide)
    args = (
        logits, token_ids, response_mask, lengths, prompt_of, old_logprob, ref, advantages,
        returns, critic_hidden.reshape(all_seqs * tile, feats), value_weight,
    )
    args = tuple(pltpu.with_memory_space_constraint(x, pltpu.HBM) for x in args)
    scratch = [
        pltpu.SMEM(x.shape, x.dtype) if x.shape == (seq_rows,) else pltpu.VMEM(x.shape, x.dtype)
        for x in args
    ]
    scratch += [pltpu.VMEM((seq_len, LANES), t) for t in (F32, F32, F32, jnp.int32)]
    scratch += [
        pltpu.VMEM((n, k, wide), F32) for n, k in ((dp, 4), (tensor, 1), (tensor, 4), (dp, 1))
    ]
    dma = pltpu.SemaphoreType.DMA
    scratch += [dma((10,)), dma((seq_rows,))]
    for n in (dp, tensor, tensor, dp):
        scratch += [dma((n - 1,)), dma((n - 1,))]
    dims = (dp, tensor, seq_rows, seq_len, vocab, all_seqs, tile)
    token_loss, grad = pl.pallas_call(
        functools.partial(kernel, dims),
        out_shape=(
            jax.ShapeDtypeStruct((seq_rows, seq_len), F32),
            jax.ShapeDtypeStruct((wide, feats), BF16),
        ),
        in_specs=[pl.BlockSpec(memory_space=pltpu.HBM)] * len(args),
        out_specs=(pl.BlockSpec(memory_space=pltpu.VMEM), pl.BlockSpec(memory_space=pltpu.VMEM)),
        scratch_shapes=scratch,
        compiler_params=pltpu.CompilerParams(
            collective_id=0, has_side_effects=True, vmem_limit_bytes=16 << 20
        ),
        name="ppo",
    )(*args)
    token_loss, grad = pl.pallas_call(
        write_out,
        out_shape=(
            jax.ShapeDtypeStruct((seq_rows, seq_len), F32),
            jax.ShapeDtypeStruct((wide, feats), BF16),
        ),
        in_specs=[pl.BlockSpec(memory_space=pltpu.VMEM)] * 2,
        out_specs=(pl.BlockSpec(memory_space=pltpu.HBM),) * 2,
        scratch_shapes=[dma((PIECES + 1,))],
        compiler_params=pltpu.CompilerParams(vmem_limit_bytes=16 << 20),
        name="tail",
    )(token_loss, grad)
    return token_loss, grad.reshape(all_seqs, tile, feats)


def solution(mesh):
    in_specs = (
        P("dp", None, "tensor"),
        P("dp", None),
        P("dp", None),
        P("dp"),
        P("dp"),
        P("dp", None),
        P(None, "dp"),
        P("dp", None),
        P("dp", None),
        P(None, "dp", "tensor"),
        P("tensor"),
    )
    out_specs = (P("dp", None), P(None, "dp", "tensor"))
    return jax.shard_map(
        per_device, mesh=mesh, in_specs=in_specs, out_specs=out_specs, check_vma=False
    )
```

```python
import functools

import jax
import jax.numpy as jnp
from jax import lax
from jax.experimental import pallas as pl
from jax.experimental.pallas import tpu as pltpu
from jax.sharding import PartitionSpec as P

F32 = jnp.float32
BF16 = jnp.bfloat16
MESH = pl.DeviceIdType.MESH
LANES = 128
ROWS = 32
PIECES = 4


def select_dot(x, hot):
    hi = x.astype(BF16)
    rest = x - hi.astype(F32)
    mid = rest.astype(BF16)
    low = (rest - mid.astype(F32)).astype(BF16)
    n = x.shape[0]
    out = jnp.dot(jnp.concatenate([hi, mid, low], axis=0), hot, preferred_element_type=F32)
    return out[:n] + out[n : 2 * n] + out[2 * n :]


def kernel(
    dims,
    logits_hbm, ids_hbm, mask_hbm, len_hbm, prompt_hbm, old_hbm, ref_hbm, adv_hbm, ret_hbm,
    hidden_hbm, weight_hbm,
    loss_ref, grad_ref,
    logits, ids, mask, lens, prompts, old, ref, adv, ret, hidden, weight,
    top_col, sum_col, hit_col, id_col,
    early, value_part, stats, value_sum,
    in_sem, logit_sem,
    e_send, e_recv, v_send, v_recv, s_send, s_recv, w_send, w_recv,
):
    dp, tensor, seq_rows, seq_len, vocab, all_seqs, tile = dims
    wide = seq_rows * seq_len
    me_dp = lax.axis_index("dp")
    me_t = lax.axis_index("tensor")

    smalls = [
        pltpu.make_async_copy(src, dst, in_sem.at[n])
        for n, (src, dst) in enumerate(
            [
                (hidden_hbm, hidden), (weight_hbm, weight), (ids_hbm, ids), (mask_hbm, mask),
                (len_hbm, lens), (prompt_hbm, prompts), (ref_hbm, ref), (adv_hbm, adv),
                (ret_hbm, ret), (old_hbm, old),
            ]
        )
    ]
    bigs = [
        pltpu.make_async_copy(logits_hbm.at[r], logits.at[r], logit_sem.at[r])
        for r in range(seq_rows)
    ]
    for c in smalls[:2]:
        c.start()
    barrier = pltpu.get_barrier_semaphore()
    for d in range(1, dp):
        pl.semaphore_signal(
            barrier, inc=1, device_id=(lax.rem(me_dp + d, dp), me_t), device_id_type=MESH
        )
    for d in range(1, tensor):
        pl.semaphore_signal(
            barrier, inc=1, device_id=(me_dp, lax.rem(me_t + d, tensor)), device_id_type=MESH
        )
    for c in smalls[2:] + bigs:
        c.start()

    def over_dp(buf, send, recv):
        return [
            pltpu.make_async_remote_copy(
                src_ref=buf.at[me_dp], dst_ref=buf.at[me_dp],
                send_sem=send.at[d - 1], recv_sem=recv.at[d - 1],
                device_id=(lax.rem(me_dp + d, dp), me_t), device_id_type=MESH,
            )
            for d in range(1, dp)
        ]

    def over_tensor(buf, send, recv):
        return [
            pltpu.make_async_remote_copy(
                src_ref=buf.at[me_t], dst_ref=buf.at[me_t],
                send_sem=send.at[d - 1], recv_sem=recv.at[d - 1],
                device_id=(me_dp, lax.rem(me_t + d, tensor)), device_id_type=MESH,
            )
            for d in range(1, tensor)
        ]

    e_copies = over_dp(early, e_send, e_recv)
    v_copies = over_tensor(value_part, v_send, v_recv)
    s_copies = over_tensor(stats, s_send, s_recv)
    w_copies = over_dp(value_sum, w_send, w_recv)

    smalls[0].wait()
    smalls[1].wait()
    head_row = weight[...].reshape(1, weight.shape[0])
    head = jnp.broadcast_to(head_row, (16, weight.shape[0]))
    part = lax.dot_general(
        head, hidden[...], (((1,), (1,)), ((), ())), preferred_element_type=F32
    )
    value_part[me_t] = part[:1]
    pl.semaphore_wait(barrier, dp - 1 + tensor - 1)
    for c in v_copies:
        c.start()

    for c in smalls[2:]:
        c.wait()

    def flat(x):
        return jnp.concatenate([x[r : r + 1] for r in range(seq_rows)], axis=1)

    lane = lax.broadcasted_iota(jnp.int32, (1, wide), 1)
    seq_of = lane // seq_len
    len_row = jnp.zeros((1, wide), jnp.int32)
    prompt_row = jnp.zeros((1, wide), jnp.int32)
    for r in range(seq_rows):
        len_row = jnp.where(seq_of == r, lens[r], len_row)
        prompt_row = jnp.where(seq_of == r, prompts[r], prompt_row)
    live = (flat(mask[...]) * (lane % seq_len < len_row).astype(jnp.int32)).astype(F32)
    adv_row = flat(adv[...])
    ret_row = flat(ret[...])
    if tile % 16 == 0:
        spread = (
            lax.broadcasted_iota(jnp.int32, (tile, wide), 0)
            == lax.broadcasted_iota(jnp.int32, (tile, wide), 1) % tile
        ).astype(F32).astype(BF16)
        ref_wide = jnp.dot(ref[...], spread, preferred_element_type=F32)
        owner = (
            lax.broadcasted_iota(jnp.int32, (all_seqs, wide), 0)
            == lax.broadcasted_iota(jnp.int32, (all_seqs, wide), 1) // tile
        )
        ref_row = jnp.sum(jnp.where(owner, ref_wide, 0.0), axis=0, keepdims=True)
    else:
        ref_row = ref[...].astype(F32)
    code = live * (prompt_row.astype(F32) + 1.0)
    early[me_dp] = jnp.concatenate([ret_row, code, adv_row, ref_row], axis=0)
    for c in e_copies:
        c.start()

    start = me_t * vocab
    lane_block = lax.broadcasted_iota(jnp.int32, (ROWS, LANES), 1)

    def column(row):
        return jnp.broadcast_to(row, (LANES, LANES)).T

    def logit_pass(r):
        bigs[r].wait()
        for h in range(seq_len // LANES):
            id_row = (ids[r : r + 1, h * LANES : (h + 1) * LANES] - start).astype(F32)
            id_col[h * LANES : (h + 1) * LANES, :] = column(id_row).astype(jnp.int32)

        def top_step(n, _):
            rows = pl.ds(pl.multiple_of(n * ROWS, ROWS), ROWS)
            top = logits[r, rows, 0:LANES]
            for c in range(1, vocab // LANES):
                top = jnp.maximum(top, logits[r, rows, c * LANES : (c + 1) * LANES])
            peak = jnp.max(top.astype(F32), axis=1, keepdims=True)
            top_col[rows, :] = jnp.broadcast_to(peak, (ROWS, LANES))
            return 0

        lax.fori_loop(0, seq_len // ROWS, top_step, 0, unroll=True)

        def sum_step(n, _):
            rows = pl.ds(pl.multiple_of(n * ROWS, ROWS), ROWS)
            peak = top_col[rows, :]
            want = id_col[rows, :]
            total = jnp.zeros((ROWS, LANES), F32)
            hit = jnp.zeros((ROWS, LANES), F32)
            for c in range(vocab // LANES):
                x = logits[r, rows, c * LANES : (c + 1) * LANES].astype(F32)
                total = total + jnp.exp(x - peak)
                hit = jnp.where(lane_block + c * LANES == want, x, hit)
            sum_col[rows, :] = total
            hit_col[rows, :] = hit
            return 0

        lax.fori_loop(0, seq_len // ROWS, sum_step, 0)
        for h in range(seq_len // LANES):
            rows = slice(h * LANES, (h + 1) * LANES)
            cols = slice(r * seq_len + h * LANES, r * seq_len + (h + 1) * LANES)
            stats[me_t, 0:1, cols] = top_col[rows, :].T[0:1]
            stats[me_t, 1:2, cols] = jnp.sum(sum_col[rows, :].T, axis=0, keepdims=True)
            stats[me_t, 2:3, cols] = jnp.sum(hit_col[rows, :].T, axis=0, keepdims=True)

    stats[me_t, 3:4, :] = jnp.zeros((1, wide), F32)
    for r in range(seq_rows):
        logit_pass(r)
    for c in s_copies:
        c.start()

    for c in v_copies:
        c.wait_recv()
    value = value_part[0]
    for j in range(1, tensor):
        value = value + value_part[j]
    value_sum[me_dp] = value
    for c in w_copies:
        c.start()

    for c in e_copies:
        c.wait_recv()
    k = lax.broadcasted_iota(jnp.int32, (wide, wide), 0)
    l = lax.broadcasted_iota(jnp.int32, (wide, wide), 1)
    to_tile = (k == ((l // tile) % seq_rows) * seq_len + me_dp * tile + l % tile).astype(F32)
    to_seq = (k == (me_dp * seq_rows + l // seq_len) * tile + l % tile).astype(F32)
    to_seq = to_seq.astype(BF16)
    row_id = lax.broadcasted_iota(jnp.int32, (dp, wide), 0)
    lane_id = lax.broadcasted_iota(jnp.int32, (dp, wide), 1)
    from_seq = row_id == lane_id // (tile * seq_rows)
    from_tile = row_id == (lane_id % seq_len) // tile

    def fold(x, keep):
        return jnp.sum(jnp.where(keep, x, 0.0), axis=0, keepdims=True)

    code_all = early[:, 1, :]
    live_all = jnp.where(code_all > 0.0, 1.0, 0.0)
    moved = select_dot(
        jnp.concatenate([early[:, 0, :], live_all], axis=0), to_tile.astype(BF16)
    )
    ret_tile = fold(moved[:dp], from_seq)
    live_tile = fold(moved[dp:], from_seq)
    ref_seq = fold(
        jnp.dot(early[:, 3, :].astype(BF16), to_seq, preferred_element_type=F32), from_tile
    )

    coeff = 32.0 * live_tile * (value - ret_tile)
    head32 = head_row.astype(F32)
    for h in range(wide // LANES):
        factor = column(coeff[:, h * LANES : (h + 1) * LANES])
        for c in range(head32.shape[1] // LANES):
            cols = slice(c * LANES, (c + 1) * LANES)
            grad_ref[h * LANES : (h + 1) * LANES, cols] = (factor * head32[:, cols]).astype(BF16)

    adv_all = early[:, 2, :]
    whitened = jnp.zeros((1, wide), F32)
    for r in range(seq_rows):
        same = jnp.where(code_all == prompts[r].astype(F32) + 1.0, 1.0, 0.0)
        count = jnp.maximum(jnp.sum(same, keepdims=True), 1.0)
        mean = jnp.sum(same * adv_all, keepdims=True) / count
        off = adv_all - mean
        var = jnp.sum(same * off * off, keepdims=True) / count
        whitened = jnp.where(seq_of == r, (adv_row - mean) * lax.rsqrt(var + 1.0), whitened)

    for c in s_copies:
        c.wait_recv()
    row_max = stats[0, 0:1]
    for j in range(1, tensor):
        row_max = jnp.maximum(row_max, stats[j, 0:1])
    total = jnp.zeros((1, wide), F32)
    target = jnp.zeros((1, wide), F32)
    for j in range(tensor):
        total = total + stats[j, 1:2] * jnp.exp(stats[j, 0:1] - row_max)
        target = target + stats[j, 2:3]
    logprob = target - (row_max + jnp.log(total))
    prob_ratio = jnp.exp(jnp.clip(logprob - flat(old[...]), -20.0, 20.0))
    surrogate = jnp.maximum(-whitened * prob_ratio, -whitened * jnp.clip(prob_ratio, 0.8, 1.2))
    surrogate = jnp.where(whitened < 0.0, jnp.minimum(surrogate, -3.0 * whitened), surrogate)
    drift = jnp.clip(ref_seq - logprob, -20.0, 20.0)
    penalty = jnp.clip(jnp.exp(drift) - drift - 1.0, -10.0, 10.0)
    policy = surrogate + 0.1 * penalty

    for c in w_copies:
        c.wait_recv()
    value_seq = fold(select_dot(value_sum[:, 0, :], to_seq), from_tile)
    error = value_seq - ret_row
    loss = live * (policy + 0.25 * error * error)
    for r in range(seq_rows):
        loss_ref[r : r + 1, :] = loss[:, r * seq_len : (r + 1) * seq_len]
    for c in v_copies + e_copies + s_copies + w_copies:
        c.wait_send()


def write_out(loss_in, grad_in, loss_ref, grad_ref, sems):
    copies = [pltpu.make_async_copy(loss_in, loss_ref, sems.at[0])]
    step = grad_in.shape[0] // PIECES
    for n in range(PIECES):
        rows = pl.ds(n * step, step)
        copies.append(
            pltpu.make_async_copy(grad_in.at[rows], grad_ref.at[rows], sems.at[n + 1])
        )
    for c in copies:
        c.start()
    for c in copies:
        c.wait()


def per_device(
    logits, token_ids, response_mask, lengths, prompt_of, old_logprob, ref_logprob, advantages,
    returns, critic_hidden, value_weight,
):
    seq_rows, seq_len, vocab = logits.shape
    all_seqs, tile, feats = critic_hidden.shape
    dp = lax.axis_size("dp")
    tensor = lax.axis_size("tensor")
    wide = seq_rows * seq_len
    ref = ref_logprob if tile % 16 == 0 else ref_logprob.reshape(1, wide)
    args = (
        logits, token_ids, response_mask, lengths, prompt_of, old_logprob, ref, advantages,
        returns, critic_hidden.reshape(all_seqs * tile, feats), value_weight,
    )
    args = tuple(pltpu.with_memory_space_constraint(x, pltpu.HBM) for x in args)
    scratch = [
        pltpu.SMEM(x.shape, x.dtype) if x.shape == (seq_rows,) else pltpu.VMEM(x.shape, x.dtype)
        for x in args
    ]
    scratch += [pltpu.VMEM((seq_len, LANES), t) for t in (F32, F32, F32, jnp.int32)]
    scratch += [
        pltpu.VMEM((n, k, wide), F32) for n, k in ((dp, 4), (tensor, 1), (tensor, 4), (dp, 1))
    ]
    dma = pltpu.SemaphoreType.DMA
    scratch += [dma((10,)), dma((seq_rows,))]
    for n in (dp, tensor, tensor, dp):
        scratch += [dma((n - 1,)), dma((n - 1,))]
    dims = (dp, tensor, seq_rows, seq_len, vocab, all_seqs, tile)
    token_loss, grad = pl.pallas_call(
        functools.partial(kernel, dims),
        out_shape=(
            jax.ShapeDtypeStruct((seq_rows, seq_len), F32),
            jax.ShapeDtypeStruct((wide, feats), BF16),
        ),
        in_specs=[pl.BlockSpec(memory_space=pltpu.HBM)] * len(args),
        out_specs=(pl.BlockSpec(memory_space=pltpu.VMEM), pl.BlockSpec(memory_space=pltpu.VMEM)),
        scratch_shapes=scratch,
        compiler_params=pltpu.CompilerParams(
            collective_id=0, has_side_effects=True, vmem_limit_bytes=16 << 20
        ),
        name="ppo",
    )(*args)
    token_loss, grad = pl.pallas_call(
        write_out,
        out_shape=(
            jax.ShapeDtypeStruct((seq_rows, seq_len), F32),
            jax.ShapeDtypeStruct((wide, feats), BF16),
        ),
        in_specs=[pl.BlockSpec(memory_space=pltpu.VMEM)] * 2,
        out_specs=(pl.BlockSpec(memory_space=pltpu.HBM),) * 2,
        scratch_shapes=[dma((PIECES + 1,))],
        compiler_params=pltpu.CompilerParams(vmem_limit_bytes=16 << 20),
        name="tail",
    )(token_loss, grad)
    return token_loss, grad.reshape(all_seqs, tile, feats)


def solution(mesh):
    in_specs = (
        P("dp", None, "tensor"),
        P("dp", None),
        P("dp", None),
        P("dp"),
        P("dp"),
        P("dp", None),
        P(None, "dp"),
        P("dp", None),
        P("dp", None),
        P(None, "dp", "tensor"),
        P("tensor"),
    )
    out_specs = (P("dp", None), P(None, "dp", "tensor"))
    return jax.shard_map(
        per_device, mesh=mesh, in_specs=in_specs, out_specs=out_specs, check_vma=False
    )
```
